256 devices in a mesh: fsdp: 8 (over y, core), sp: 32 (over z, x).
Axes of the slice: x: 4, y: 4, z: 8, core: 2. Of those that a mesh axis runs over, the one named last changes fastest.
Arguments:
- hidden: bfloat16 [8192, 8192], P('sp', 'fsdp'), may hold values from -23 to 23
- w_query: bfloat16 [8192, 4096], P('fsdp', 'sp'), may hold values from -0.125 to 0.125
- w_keyvalue: bfloat16 [8192, 1024], P('fsdp', 'sp'), may hold values from -0.125 to 0.125
- w_output: bfloat16 [4096, 8192], P('sp', 'fsdp'), may hold values from -0.375 to 0.375
- segment_ids: int32 [8192], P('sp'), may hold values from 0 to 7, never falling along the last dimension, each value on 1 to 2048 neighbouring positions
Outputs:
- attended: bfloat16 [8192, 8192], P('sp', 'fsdp')
The draws below stay inside these ranges and needn't reach their ends.
Inputs may be any that keep to these rules, and one draw needn't show every extreme that they name: `segment_ids`: segment ids never fall along the sequence; every episode has between 1 and 2048 tokens.
All inputs are finite; a program needn't handle non-finite values.
Results may differ from the reference program's by a relative error of at most 0.0085.
The reference program's roundings to bfloat16 on the way count: a program that leaves them out, or rounds other values in their place, can miss the bound.
Values may be sent and summed in bfloat16 or wider, within the bound.
A program may use at most 128 MiB of HBM per device.

```python
import math
import jax
import jax.numpy as jnp
import numpy as np
from jax import lax

D = 8192
HD = 128
GROUP = 8
HEADS = 32
KV_HEADS = 4
SEQ = 8192


def draw_hidden(key, part):
    base_key = jax.random.fold_in(jax.random.fold_in(key, 11), 0)
    entries = jnp.clip(jax.random.normal(base_key, (SEQ, D), jnp.float32), -6.0, 6.0)
    return entries.astype(jnp.bfloat16)


def steps_of(own_key, shape, pieces, low, largest):
    def one(position, blocks):
        heights = jax.random.uniform(jax.random.fold_in(jax.random.fold_in(own_key, 6), position), (blocks,), jnp.float32, low / len(pieces), largest / len(pieces))
        return jnp.repeat(jnp.exp(heights), shape[position] // blocks).reshape((-1,) + (1,) * (len(shape) - position - 1))

    loudness = one(*pieces[0])
    for cut in pieces[1:]:
        loudness = loudness * one(*cut)
    return loudness


def profile(count, total, limit, slope):
    weights = [(1 << 20) // math.isqrt(grade ** slope) + 1 for grade in range(2, count + 1)]
    surplus, holding = total - limit - (count - 1), [1] * (count - 1)
    while surplus > 0:
        candidates = [i for i in range(count - 1) if holding[i] < limit]
        pool, remaining = sum([weights[i] for i in candidates]), surplus
        for i in candidates:
            addition = min(limit - holding[i], max(1, remaining * weights[i] // pool), surplus)
            holding[i] = holding[i] + addition
            surplus = surplus - addition
    return np.array([limit] + holding)


def ragged_sizes(own_key, number_of, total, reach, skew):
    if number_of == 2:
        one = jax.random.randint(own_key, (), max(1, total - reach), min(reach, total - 1) + 1)
        return jnp.stack([one, total - one])
    lengths = jnp.asarray(profile(number_of, total, reach, skew), jnp.int32)
    couples = (number_of - 1) // 2
    source_of, sink = lengths[1:1 + 2 * couples:2], lengths[2:2 + 2 * couples:2]
    room = jnp.minimum(source_of - 1, reach - sink)
    shifted = jax.random.randint(jax.random.fold_in(own_key, 1), (couples,), 0, 1 << 20) % (room + 1)
    lengths = lengths.at[1:1 + 2 * couples:2].set(source_of - shifted).at[2:2 + 2 * couples:2].set(sink + shifted)
    return lengths[jax.random.permutation(jax.random.fold_in(own_key, 2), number_of)]


def scatter_about(own_key, dims, spread, bound, pieces=(), held_as=jnp.bfloat16):
    values = jax.random.normal(own_key, dims, jnp.float32) * spread
    if len(pieces) > 0:
        values = steps_of(own_key, dims, pieces, -0.22, 0.18) * values
    return jnp.clip(values, min=-bound, max=bound).astype(held_as)


def setup_inputs(seed: int = 0) -> dict:
    arg_keys = jax.random.split(jax.random.key(seed), 6)
    return {
        "hidden": draw_hidden(jax.random.fold_in(arg_keys[5], 71), 0),
        "w_query": scatter_about(arg_keys[1], (D, HEADS * HD), (D // 4) ** -0.5, 0.125, ((0, 8), (1, 32))),
        "w_keyvalue": scatter_about(arg_keys[2], (D, 2 * KV_HEADS * HD), (D // 4) ** -0.5, 0.125, ((0, 8), (1, 32))),
        "w_output": scatter_about(arg_keys[3], (HEADS * HD, D), (HEADS * HD // 16) ** -0.5, 0.375, ((0, 32), (1, 8))),
        "segment_ids": jnp.searchsorted(jnp.cumsum(ragged_sizes(arg_keys[4], 8, SEQ, SEQ // 4, 0)), jnp.arange(SEQ), side="right").astype(jnp.int32),
    }


ROPE_BASE = 500000.0
NEG_FILL = -1.0e30


def rotate(values, positions, head_count, width):
    row_count = values.shape[0]
    shaped = values.reshape(row_count, head_count, width)
    half_width = width // 2
    frequency = jnp.exp(jnp.arange(half_width, dtype=jnp.float32) * (-2.0 * math.log(ROPE_BASE) / width))
    angles = positions.astype(jnp.float32)[:, None] * frequency[None, :]
    cosine = jnp.cos(angles)[:, None, :]
    sine_part = jnp.sin(angles)[:, None, :]
    lower_half = shaped[:, :, :half_width]
    upper_half = shaped[:, :, half_width:]
    turned = jnp.concatenate([lower_half * cosine - upper_half * sine_part, upper_half * cosine + lower_half * sine_part], axis=2)
    return turned.reshape(row_count, head_count * width)


def split_keys(kv_sum, positions, kv_count, width):
    row_count = kv_sum.shape[0]
    shaped = kv_sum.reshape(row_count, kv_count, 2, width)
    key_part = rotate(shaped[:, :, 0, :].reshape(row_count, kv_count * width), positions, kv_count, width)
    key_part = key_part.reshape(row_count, kv_count, 1, width)
    return jnp.concatenate([key_part, shaped[:, :, 1:2, :]], axis=2).astype(jnp.bfloat16)


def reference(hidden, w_query, w_keyvalue, w_output, segment_ids):
    seq_len = hidden.shape[0]
    positions = jnp.arange(seq_len, dtype=jnp.int32)
    query = rotate(jnp.dot(hidden, w_query, preferred_element_type=jnp.float32), positions, HEADS, HD).astype(jnp.bfloat16)
    pairs = split_keys(jnp.dot(hidden, w_keyvalue, preferred_element_type=jnp.float32), positions, KV_HEADS, HD)
    key_all = pairs[:, :, 0, :]
    value_all = pairs[:, :, 1, :]
    block_len = min(512, seq_len)
    block_count = seq_len // block_len
    score_scale = HD ** -0.5

    def one_block(item_index):
        head_id = item_index // block_count
        block_id = item_index % block_count
        first_row = (block_id * block_len).astype(jnp.int32)
        query_block = lax.dynamic_slice(query, (first_row, (head_id * HD).astype(jnp.int32)), (block_len, HD))
        group_id = (head_id // GROUP).astype(jnp.int32)
        key_block = lax.dynamic_index_in_dim(key_all, group_id, axis=1, keepdims=False)
        value_block = lax.dynamic_index_in_dim(value_all, group_id, axis=1, keepdims=False)
        scores = lax.dot_general(query_block, key_block, (((1,), (1,)), ((), ())), preferred_element_type=jnp.float32) * score_scale
        query_pos = first_row + jnp.arange(block_len, dtype=jnp.int32)
        query_seg = lax.dynamic_slice_in_dim(segment_ids, first_row, block_len)
        allowed = (positions[None, :] <= query_pos[:, None]) & (segment_ids[None, :] == query_seg[:, None])
        masked = jnp.where(allowed, scores, NEG_FILL)
        row_max = jnp.max(masked, axis=1, keepdims=True)
        weights = jnp.where(allowed, jnp.exp(masked - row_max), 0.0)
        row_total = jnp.sum(weights, axis=1, keepdims=True)
        mixed_block = jnp.dot(weights.astype(jnp.bfloat16), value_block, preferred_element_type=jnp.float32)
        return (mixed_block / row_total).astype(jnp.bfloat16)

    blocks = lax.map(one_block, jnp.arange(HEADS * block_count, dtype=jnp.int32))
    mixed = blocks.reshape(HEADS, seq_len, HD).transpose(1, 0, 2).reshape(seq_len, HEADS * HD)
    return jnp.dot(mixed, w_output, preferred_element_type=jnp.float32).astype(jnp.bfloat16)
```

```python
import functools
import math

import jax
import jax.numpy as jnp
import numpy as np
from jax import lax
from jax.experimental import pallas as pl
from jax.experimental.pallas import tpu as pltpu
from jax.sharding import Mesh
from jax.sharding import PartitionSpec as P

HD = 128
HALF = HD // 2
ROPE_BASE = 500000.0
NEG_FILL = -1e30
SEGMENTS = 8
CODES = 32000.0
MESH = pl.DeviceIdType.MESH
F32 = jnp.float32
BF16 = jnp.bfloat16


def dot(a, b):
    return lax.dot_general(a, b, (((1,), (0,)), ((), ())), preferred_element_type=F32)


def dot_nt(a, b):
    return lax.dot_general(a, b, (((1,), (1,)), ((), ())), preferred_element_type=F32)


def kernel(
    dims,
    h_hbm, wq_hbm, wk_hbm, wo_hbm, seg_hbm, freq_hbm, out,
    h, wk, seg, freq, hb, wb, wob, wk2, kvw, pq, rq, pk, rk, sq, yq, acc_q, sk, yk, sk_unit, yk_unit, sq_unit, yq_unit, acc_k,
    seg_win, cos_q, sin_q, qs, mix, send_part, recv_part, relay_out, relay_in, acc_o,
    sem_local, h_s, h_r, sw_s, sw_r, w_s, wk_s, w_r, wo_s, wo_r, d_s, d_r, dk_s, dk_r,
    yq_s, yq_r, yk_s, yk_r, yu_s, yu_r, sg_s, sg_r, kz_s, kz_r, kx_s, kx_r, kc_s, kc_r,
    my_s, my_r, mc_s, mc_r, xr_s, xr_r, xf_s, xf_r,
):
    ny, nz, tb, kd, nc = dims
    nx = 4
    zh = nz // 2
    block = nx * tb
    th = tb // 2
    x = lax.axis_index("x")
    y = lax.axis_index("y")
    z = lax.axis_index("z")
    c = lax.axis_index("c")
    named = jax.named_scope

    def x_at(d):
        return {"x": lax.rem(x + d + nx, nx)}

    def z_at(d):
        return {"z": lax.rem(z + d + nz, nz)}

    def y_at(d):
        return {"y": lax.rem(y + d + ny, ny)}

    partner = {"c": 1 - c}

    def rc(src, dst, ssem, rsem, dev):
        return pltpu.make_async_remote_copy(
            src_ref=src, dst_ref=dst, send_sem=ssem, recv_sem=rsem, device_id=dev, device_id_type=MESH
        )

    def go(cp):
        cp.start()
        return cp

    def whole(ref, ssem, rsem):
        return rc(ref, ref, ssem, rsem, {"c": 1 - c})

    hi = lax.div(x, 2)
    lanes = (pl.ds(0, HD), pl.ds(HD, HD))
    own_lanes = pl.ds(pl.multiple_of(2 * block + x * tb, tb), tb)
    own_rows = pl.ds(pl.multiple_of(z * HD, HD), HD)
    local = {
        "wk": pltpu.make_async_copy(wk_hbm, wk, sem_local.at[0]),
        "wk_own": pltpu.make_async_copy(wk_hbm.at[hi], wk2.at[0, hi], sem_local.at[1]),
        "wq": pltpu.make_async_copy(wq_hbm, wb.at[0, :, lanes[0]], sem_local.at[2]),
        "h": pltpu.make_async_copy(h_hbm, h, sem_local.at[3]),
        "seg": pltpu.make_async_copy(seg_hbm, seg, sem_local.at[4]),
        "seg_own": pltpu.make_async_copy(seg_hbm, seg_win.at[:, own_lanes], sem_local.at[5]),
        "freq": pltpu.make_async_copy(freq_hbm, freq, sem_local.at[6]),
        "wo": pltpu.make_async_copy(wo_hbm, wob.at[own_rows, :], sem_local.at[7]),
    }
    for cp in local.values():
        cp.start()

    barrier = pltpu.get_barrier_semaphore()
    greet = [x_at(d) for d in range(1, nx)] + [z_at(1), z_at(-1), z_at(2), z_at(-2), partner]
    greet += [y_at(d) for d in range(1, ny)]
    for dev in greet:
        pl.semaphore_signal(barrier, inc=1, device_id=dev, device_id_type=MESH)
    for name in ("wk", "wq", "h"):
        local[name].wait()
    with named("barrier"):
        pl.semaphore_wait(barrier, len(greet))

    swap = go(rc(wk.at[1 - hi], wk2.at[0, hi], sw_s, sw_r, x_at(2)))

    k_rows = (pl.ds(0, kd // 2), pl.ds(kd // 2, kd // 2))

    def w_copy(r, way, piece):
        rows = k_rows[piece]
        dst = wb.at[0, rows, lanes[1]] if r == zh else wb.at[r, rows, lanes[1 - way]]
        src = wb.at[0, rows, lanes[0]] if r == 1 else wb.at[r - 1, rows, lanes[1 - way]]
        return rc(src, dst, w_s, w_r.at[r - 1, way, piece], z_at(1 - 2 * way))

    def k_copy(r, way):
        part = pl.ds(0, 2)
        if r == zh:
            part = pl.ds(way, 1)
            dst = wk2.at[zh, part]
        else:
            dst = wk2.at[nz - r if way == 0 else r, part]
        src_at = 0 if r == 1 else (nz - r + 1 if way == 0 else r - 1)
        src = wk2.at[src_at, part]
        return rc(src, dst, wk_s, w_r.at[r - 1, way, 2], z_at(1 - 2 * way))

    def pieces(r, way):
        return (way,) if r == zh else (0, 1)

    w_cp = {}

    def k_step(r):
        for way in range(2):
            w_cp[r, way, 2].wait_recv()
            if r < zh:
                w_cp[r + 1, way, 2] = go(k_copy(r + 1, way))

    def w_step(r, piece):
        for way in range(2):
            if piece in pieces(r, way):
                w_cp[r, way, piece].wait_recv()
                if r < zh and piece in pieces(r + 1, way):
                    w_cp[r + 1, way, piece] = go(w_copy(r + 1, way, piece))

    h_rows = (pl.ds(0, th), pl.ds(th, th))
    for way in range(2):
        w_cp[1, way, 0] = go(w_copy(1, way, 0))
    for k in range(2):
        go(rc(h.at[h_rows[k]], hb.at[2, h_rows[k]], h_s, h_r.at[0, k], x_at(1)))
        go(rc(h.at[h_rows[1 - k]], hb.at[0, h_rows[1 - k]], h_s, h_r.at[1, k], x_at(-1)))

    local["seg"].wait()
    local["seg_own"].wait()
    local["freq"].wait()
    local["wk_own"].wait()

    def seg_x(d):
        return rc(seg, seg_win.at[:, own_lanes], sg_s, sg_r.at[0], x_at(d))

    for d in range(1, nx):
        go(seg_x(d))

    def blk(b):
        return pl.ds((2 - b) * block, block)

    def seg_z(b):
        return rc(seg_win.at[:, blk(0)], seg_win.at[:, blk(b)], sg_s, sg_r.at[1], z_at(b))

    row = lax.broadcasted_iota(jnp.int32, (block, HD), 0)
    pos = (z * block + row).astype(F32)
    angle = pos * freq[4 * 16:4 * 16 + 1, :]
    with named("swap"):
        swap.wait_recv()
    for way in range(2):
        w_cp[1, way, 2] = go(k_copy(1, way))
    for way in range(2):
        w_cp[1, way, 1] = go(w_copy(1, way, 1))
    with named("cos"):
        cos_q[...] = jnp.cos(angle)
    lane = lax.broadcasted_iota(jnp.int32, (block, HD), 1)
    with named("sin"):
        sin_q[...] = jnp.sin(angle) * jnp.where(lane < HALF, -1.0, 1.0)

    def h_recv(way, k):
        rows = h_rows[k] if way == 0 else h_rows[1 - k]
        return rc(h.at[rows], hb.at[2 if way == 0 else 0, rows], h_s, h_r.at[way, k], x_at(1))

    def fwd_hidden(k):
        h_recv(0, k).wait_recv()
        h_recv(1, k).wait_recv()
        if k == 0:
            go(rc(hb.at[2, h_rows[0]], hb.at[1, h_rows[0]], h_s, h_r.at[2, 0], x_at(1)))
            go(rc(hb.at[0, h_rows[1]], hb.at[1, h_rows[1]], h_s, h_r.at[2, 1], x_at(-1)))

    parity = lax.rem(z + c, 2)

    def sub(j):
        return h[...] if j == 0 else hb[j - 1]

    def rows_of(j):
        return pl.ds(pl.multiple_of(lax.rem(x + j, nx) * tb, tb), tb)

    order = (0, 1, 3, 2)
    parts = (pl.ds(0, 3), pl.ds(3, 1))

    def exchange(u, half):
        at = (slice(None), slice(None), lanes[half])
        return rc(pq.at[(u, *at)], rq.at[(u // 2, *at)], d_s, d_r.at[u // 2, half], partner)

    def project(u, js, halves=(0, 1)):
        at = pl.ds(halves[0] * HD, len(halves) * HD)
        for j in js:
            pq[u, order.index(j), :, at] = dot(sub(j), wb[u, :, at])

    def hand_over(u, halves=(0, 1)):
        @pl.when(parity != u % 2)
        def _():
            for half in halves:
                exchange(u, half).start()

    def y_copy(slot, dest):
        return rc(sq.at[slot], yq.at[slot], yq_s, yq_r, {"y": dest})

    def q_unit_y(slot, dest):
        return rc(sq_unit.at[slot], yq_unit.at[slot], yu_s.at[1], yu_r.at[1], {"y": dest})

    def deliver(u, halves=(0, 1)):
        @pl.when(parity == u % 2)
        def _():
            for half in halves:
                exchange(u, half).wait_recv()
                d = (u if half == 0 else (nz - u)) if u else (0 if half == 0 else zh)
                dest = lax.div(lax.rem(z + d, nz), 2)
                slot = lax.rem(y - dest + ny, ny) - 1

                @pl.when(dest == y)
                def _():
                    acc_q[...] = pq[u, :, :, lanes[half]] + rq[u // 2, :, :, lanes[half]]

                @pl.when(dest != y)
                def _():
                    total = pq[u, :, :, lanes[half]] + rq[u // 2, :, :, lanes[half]]
                    largest = jnp.maximum(jnp.max(jnp.abs(total), keepdims=True), 1e-33)
                    sq_unit[slot] = jnp.broadcast_to(largest.reshape(1, 1) * (1.0 / CODES), (8, HD))
                    q_unit_y(slot, dest).start()
                    sq[slot] = jnp.round(total * (CODES / largest)).astype(jnp.int32).astype(jnp.int16)
                    y_copy(slot, dest).start()

    rows_k = nz * 2 * 16

    def k_project(js):
        wk_all = wk2[...].reshape(rows_k, kd)
        for j in js:
            pk[:, order.index(j)] = dot_nt(wk_all, sub(j)).reshape(nz, 2, 16, tb)

    turns = (1, 3, 2, 0)

    def k_chunk(turn, core):
        return lax.rem(2 * lax.rem(y + turn, ny) + core - z + nz, nz)

    def k_exchange(turn, p):
        return rc(
            pk.at[k_chunk(turn, 1 - c), parts[p]], rk.at[turn, parts[p]], dk_s, dk_r.at[turn, p], partner
        )

    def k_hand_over(p):
        for turn in turns:
            k_exchange(turn, p).start()

    def k_copy_y(slot, p, dest):
        return rc(sk.at[slot, parts[p]], yk.at[slot, parts[p]], yk_s, yk_r, {"y": dest})

    def k_unit_y(slot, p, dest):
        return rc(sk_unit.at[slot, p], yk_unit.at[slot, p], yu_s.at[0], yu_r.at[0], {"y": dest})

    def k_deliver(p):
        for turn in turns:
            k_exchange(turn, p).wait_recv()
            dest = lax.rem(y + turn, ny)
            slot = ny - turn - 1
            total = pk[k_chunk(turn, c), parts[p]] + rk[turn, parts[p]]
            if turn == 0:
                acc_k[parts[p]] = total
            else:
                largest = jnp.maximum(jnp.max(jnp.abs(total), keepdims=True), 1e-33)
                sk_unit[slot, p] = jnp.broadcast_to(largest.reshape(1, 1) * (1.0 / CODES), (8, HD))
                k_unit_y(slot, p, dest).start()
                sk[slot, parts[p]] = jnp.round(total * (CODES / largest)).astype(jnp.int32).astype(jnp.int16)
                k_copy_y(slot, p, dest).start()

    def y_other():
        return lax.rem(y + 1, ny)

    o_cols = nc // 2

    def o_copy(r, way, piece):
        owner = lax.rem(z + (nz - r + 1 if way == 0 else r - 1), nz)
        at = wob.at[pl.ds(pl.multiple_of(owner * HD, HD), HD), pl.ds(piece * o_cols, o_cols)]
        return rc(at, at, wo_s, wo_r.at[r - 1, way, piece], z_at(1 - 2 * way))

    def o_step(r, piece, ways=(0, 1)):
        for way in ways:
            if r == 0:
                go(o_copy(1, way, piece))
            elif r < zh or way == 1:
                o_copy(r, way, piece).wait_recv()
                if r + 1 < zh or (r + 1 == zh and way == 1):
                    go(o_copy(r + 1, way, piece))

    early = (0, 1, 3)
    with named("k1"):
        k_step(1)
    with named("w1a"):
        w_step(1, 0)
    with named("hidden0"):
        fwd_hidden(0)
    with named("k2"):
        k_step(2)
    with named("w1b"):
        w_step(1, 1)
    with named("hidden1"):
        fwd_hidden(1)
    with named("project0a"):
        project(0, early, (0,))
    with named("k3"):
        if zh > 3:
            k_step(3)
    with named("w2a"):
        w_step(2, 0)
    with named("project1a"):
        project(1, early)
    whole(seg_win.at[:, pl.ds(0, 3 * tb)], sg_s, sg_r.at[0]).wait_recv()
    for b in (1, 2):
        go(seg_z(b))
    with named("w2b"):
        w_step(2, 1)
    with named("k4"):
        k_step(zh)
    with named("kproject_a"):
        k_project(early)
        k_hand_over(0)
    with named("hidden2"):
        for k in range(2):
            rc(h.at[h_rows[k]], hb.at[1, h_rows[k]], h_s, h_r.at[2, k], x_at(1)).wait_recv()
    with named("kproject_b"):
        k_project((2,))
        k_hand_over(1)
    with named("project1b"):
        project(1, (2,))
        hand_over(1)
    with named("kdeliver_a"):
        k_deliver(0)
    with named("project0b"):
        project(0, (2,), (0,))
        hand_over(0, (0,))
    with named("w3a"):
        w_step(3, 0)
    with named("kdeliver_b"):
        k_deliver(1)
    with named("w3b"):
        if zh > 3:
            w_step(3, 1)
    local["wo"].wait()
    o_step(0, 0)
    o_step(0, 1, (1,))
    with named("project2"):
        project(2, range(nx))
        hand_over(2)
    with named("project3"):
        if zh > 3:
            project(3, range(nx))
            hand_over(3)
    place = 2 * lax.rem(x, 2) + hi
    k_freq = freq[pl.ds(pl.multiple_of(place * 16, 16), 16), 0:1]
    is_key = c == 0
    tables = []
    for j in order:
        first = z * block + lax.rem(x + j, nx) * tb
        k_angle = (first + lax.broadcasted_iota(jnp.int32, (16, tb), 1)).astype(F32) * k_freq
        tables.append((jnp.where(is_key, jnp.cos(k_angle), 1.0), jnp.where(is_key, jnp.sin(k_angle), 0.0)))

    whole(seg_win.at[:, pl.ds(0, 2 * block)], sg_s, sg_r.at[1]).wait_recv()

    wpos = lax.broadcasted_iota(jnp.int32, (1, 3 * block), 1)
    ids = jnp.where(wpos + (z - 2) * block >= 0, seg_win[...], -1)
    starts = [jnp.sum((ids < s).astype(F32), axis=1, keepdims=True).astype(jnp.int32) for s in range(SEGMENTS)]
    with named("deliver10"):
        deliver(1)
        deliver(0, (0,))
    with named("deliver2"):
        deliver(2)
    with named("deliver3"):
        if zh > 3:
            deliver(3)
    with named("ywait_k"):
        whole(yk_unit, yu_s.at[0], yu_r.at[0]).wait_recv()
        whole(yk, yk_s, yk_r).wait_recv()
    for e, j in enumerate(order):
        total = acc_k[e]
        for s in range(ny - 1):
            unit_of = yk_unit[s, 0 if e < 3 else 1][0:1, 0:1].reshape(1, 1, 1)
            total = total + yk[s, e].astype(jnp.int32).astype(F32) * unit_of
        low, high = total[0], total[1]
        cos_e, sin_e = tables[e]
        there = pl.ds(pl.multiple_of(2 * block + lax.rem(x + j, nx) * tb, tb), tb)
        kvw[c, 0, place, :, there] = (low * cos_e - high * sin_e).astype(BF16)
        kvw[c, 1, place, :, there] = (high * cos_e + low * sin_e).astype(BF16)

    def kz(b):
        return rc(kvw.at[c, :, place, :, blk(0)], kvw.at[c, :, place, :, blk(b)], kz_s, kz_r.at[b - 1], z_at(b))

    def kx(b, d):
        at = kvw.at[c, :, place, :, blk(b)]
        return rc(at, at, kx_s, kx_r.at[b], x_at(d))

    def kx_wait(b):
        whole(kvw.at[c, :, pl.ds(0, nx - 1), :, blk(b)], kx_s, kx_r.at[b]).wait_recv()

    def kc(b):
        at = kvw.at[c, :, :, :, blk(b)]
        return rc(at, at, kc_s, kc_r.at[b], partner)

    for b in (1, 2):
        go(kz(b))
    for d in range(1, nx):
        go(kx(0, d))
    o_step(0, 1, (0,))

    with named("w4"):
        for piece in range(2):
            w_step(zh, piece)
    with named("project0c"):
        project(0, range(nx), (1,))
        hand_over(0, (1,))
    with named("deliver0"):
        deliver(0, (1,))
    with named("kz1"):
        kz(1).wait_recv()
    for d in range(1, nx):
        go(kx(1, d))
    with named("o1a"):
        o_step(1, 0)
    with named("kz2"):
        kz(2).wait_recv()
    for d in range(1, nx):
        go(kx(2, d))
    with named("o1b-"):
        o_step(1, 1, (1,))
    with named("kx0"):
        kx_wait(0)
    go(kc(0))
    with named("o2a-"):
        o_step(2, 0, (1,))
    with named("kx1"):
        kx_wait(1)
    go(kc(1))
    with named("o1b+"):
        o_step(1, 1, (0,))
    with named("kx2"):
        kx_wait(2)
    go(kc(2))
    with named("o2b-"):
        o_step(2, 1, (1,))

    with named("ywait_q"):
        whole(yq_unit, yu_s.at[1], yu_r.at[1]).wait_recv()
        whole(yq, yq_s, yq_r).wait_recv()
    with named("rope"):
        for e, j in enumerate(order):
            q = acc_q[e]
            for s in range(ny - 1):
                q = q + yq[s, e].astype(jnp.int32).astype(F32) * yq_unit[s][0:1, 0:1]
            qs[e] = (q * cos_q[rows_of(j)] + pltpu.roll(q, HALF, 1) * sin_q[rows_of(j)]).astype(BF16)
    reach = 2 * block + tb
    unit = HD**-0.5 * math.log2(math.e)
    f = 2 * y + c
    own_f = pl.ds(pl.multiple_of(f * HD, HD), HD)
    with named("kcwait"):
        for b in (0, 1, 2):
            kc(b).wait_recv()

    def attend(j):
        t = lax.rem(x + j, nx)
        at = pl.multiple_of(t * tb, tb)
        q = qs[order.index(j)]
        keys = kvw[0, :, :, :, pl.ds(at, reach)].reshape(HD, reach)
        values = kvw[1, :, :, :, pl.ds(at, reach)].reshape(HD, reach)
        scores = dot(q, keys) * unit
        here = lax.broadcasted_iota(jnp.int32, (tb, 1), 0) + 2 * block
        begin = jnp.zeros((tb, 1), jnp.int32)
        for s in starts:
            begin = jnp.maximum(begin, jnp.where(s - at <= here, s - at, 0))
        k_at = lax.broadcasted_iota(jnp.int32, (tb, reach), 1)
        ahead, own = slice(0, 2 * block), slice(2 * block, reach)
        scores = jnp.concatenate(
            [
                jnp.where(k_at[:, ahead] >= begin, scores[:, ahead], NEG_FILL),
                jnp.where((k_at[:, own] >= begin) & (k_at[:, own] <= here), scores[:, own], NEG_FILL),
            ],
            axis=1,
        )
        top = jnp.max(scores, axis=1, keepdims=True)
        weights = jnp.exp2(scores - top)
        total = jnp.sum(weights, axis=1, keepdims=True)
        mixed = dot_nt(weights.astype(BF16), values)
        mix[j, :, own_f] = (mixed / total).astype(BF16)
        for d in range(1, ny):
            go(my(j, d))
        go(mc(j, 0))

    def my(j, d):
        at = mix.at[j, :, own_f]
        return rc(at, at, my_s, my_r.at[j, d - 1], y_at(d))

    def mc(j, d):
        fd = 2 * lax.rem(y - d + ny, ny) + c
        at = mix.at[j, :, pl.ds(pl.multiple_of(fd * HD, HD), HD)]
        return rc(at, at, mc_s, mc_r.at[j], partner)

    def pass_mix(j):
        for d in range(1, ny):
            my(j, d).wait_recv()
            go(mc(j, d))

    def have_mix(j):
        whole(mix.at[j, :, pl.ds(0, ny * HD)], mc_s, mc_r.at[j]).wait_recv()

    def half_of(k):
        return pl.ds(k * th, th)

    def cols(i):
        return pl.ds(i * o_cols, o_cols)

    def relay(k, i):
        return rc(relay_out.at[k, :, cols(i)], relay_in.at[k, :, cols(i)], xr_s, xr_r.at[k, i], x_at(1 - 2 * k))

    def final(k, part, i):
        at = (k, half_of(1 - k) if part == 0 else half_of(k), cols(i))
        return rc(send_part.at[at], recv_part.at[at], xf_s, xf_r.at[i], x_at(1 - 2 * k))

    def out_dot(j, k, i):
        return dot(mix[j, half_of(k)], wob[:, cols(i)])

    with named("att2"):
        attend(2)
    with named("o2a+"):
        o_step(2, 0, (0,))
    with named("o3a-"):
        o_step(3, 0, (1,))
    with named("att1"):
        attend(1)
    with named("o2b+"):
        o_step(2, 1, (0,))
    with named("o3b-"):
        o_step(3, 1, (1,))
    with named("att3"):
        attend(3)
    with named("gm2"):
        pass_mix(2)
    with named("o4a"):
        o_step(3, 0, (0,))
        o_step(zh, 0)
    with named("mix2"):
        have_mix(2)
    with named("mm2"):
        for k in range(2):
            relay_out[k, :, cols(0)] = out_dot(2, k, 0).astype(BF16)
            go(relay(k, 0))
    with named("o4b"):
        o_step(3, 1, (0,))
        o_step(zh, 1)
    with named("mm2"):
        for k in range(2):
            relay_out[k, :, cols(1)] = out_dot(2, k, 1).astype(BF16)
            go(relay(k, 1))
    with named("gm1"):
        pass_mix(1)
    with named("att0"):
        attend(0)
    with named("mm1"):
        have_mix(1)
        for i in range(2):
            send_part[0, half_of(1), cols(i)] = out_dot(1, 1, i).astype(BF16)
            go(final(0, 0, i))
    with named("gm3"):
        pass_mix(3)
        have_mix(3)
    with named("mm3"):
        for i in range(2):
            send_part[1, half_of(0), cols(i)] = out_dot(3, 0, i).astype(BF16)
            go(final(1, 0, i))
    with named("mm31"):
        for i in range(2):
            for k, j in ((0, 1), (1, 3)):
                acc_o[k, :, cols(i)] = out_dot(j, k, i)
        pass_mix(0)
    for i in range(2):
        for k in range(2):
            with named("relay"):
                relay(k, i).wait_recv()
            send_part[k, half_of(k), cols(i)] = (acc_o[k, :, cols(i)] + relay_in[k, :, cols(i)].astype(F32)).astype(BF16)
            go(final(k, 1, i))
    with named("mm0"):
        have_mix(0)
        for i in range(2):
            for k in range(2):
                acc_o[k, :, cols(i)] = out_dot(0, k, i)

    with named("drain"):
        for ref, ssem, rsem in (
            (hb, h_s, h_r.at[0, 0]),
            (wk.at[0], sw_s, sw_r),
            (wb.at[:, pl.ds(0, kd - kd // 8)], w_s, w_r.at[0, 0, 0]),
            (wk2.at[pl.ds(0, nz - 1)], wk_s, w_r.at[0, 0, 0]),
            (wob.at[pl.ds(0, (nz - 1) * HD)], wo_s, wo_r.at[0, 0, 0]),
            (rq, d_s, d_r.at[0, 0]),
            (rk, dk_s, dk_r.at[0, 0]),
            (yq, yq_s, yq_r),
            (seg_win.at[:, pl.ds(0, 3 * tb + 2 * block)], sg_s, sg_r.at[0]),
            (kvw.at[0, :, pl.ds(0, 2), :, blk(0)], kz_s, kz_r.at[0]),
            (kvw.at[0, :, pl.ds(0, 3)], kx_s, kx_r.at[0]),
            (kvw.at[0], kc_s, kc_r.at[0]),
            (mix.at[pl.ds(0, 3), half_of(0)], my_s, my_r.at[0, 0]),
            (mix.at[pl.ds(0, 2)], mc_s, mc_r.at[0]),
            (relay_out, xr_s, xr_r.at[0, 0]),
            (send_part, xf_s, xf_r.at[0]),
        ):
            whole(ref, ssem, rsem).wait_send()

        whole(yk, yk_s, yk_r).wait_send()
        whole(yk_unit, yu_s.at[0], yu_r.at[0]).wait_send()
        whole(yq_unit, yu_s.at[1], yu_r.at[1]).wait_send()
    for i in range(2):
        with named("final"):
            whole(recv_part.at[:, :, cols(i)], xf_s, xf_r.at[i]).wait_recv()
        for k in range(2):
            rows = half_of(k)
            out[rows, cols(i)] = (
                acc_o[k, :, cols(i)] + recv_part[0, rows, cols(i)].astype(F32) + recv_part[1, rows, cols(i)].astype(F32)
            ).astype(BF16)


def on_device(ny, nz, hidden, w_query, w_keyvalue, w_output, segment_ids):
    tb, kd = hidden.shape
    nc = w_output.shape[1]
    nx, zh, block, th = 4, nz // 2, 4 * hidden.shape[0], hidden.shape[0] // 2
    freq = np.exp(np.arange(HALF, dtype=np.float32) * np.float32(-2.0 * math.log(ROPE_BASE) / HD))
    table = np.zeros((72, HD), np.float32)
    table[:HALF, 0] = freq
    table[HALF] = np.concatenate([freq, freq])
    dma = pltpu.SemaphoreType.DMA
    vm = pltpu.VMEM
    scratch = [
        vm((tb, kd), BF16),
        vm((2, 16, kd), BF16),
        vm((1, tb), jnp.int32),
        vm((72, HD), F32),
        vm((3, tb, kd), BF16),
        vm((zh, kd, 2 * HD), BF16),
        vm((nz * HD, nc), BF16),
        vm((nz, 2, 16, kd), BF16),
        vm((2, 2, 4, 16, 3 * block), BF16),
        vm((zh, nx, tb, 2 * HD), F32),
        vm((zh // 2, nx, tb, 2 * HD), F32),
        vm((nz, nx, 2, 16, tb), F32),
        vm((nz // 2, nx, 2, 16, tb), F32),
        vm((ny - 1, nx, tb, HD), jnp.int16),
        vm((ny - 1, nx, tb, HD), jnp.int16),
        vm((nx, tb, HD), F32),
        vm((ny - 1, nx, 2, 16, tb), jnp.int16),
        vm((ny - 1, nx, 2, 16, tb), jnp.int16),
        vm((ny - 1, 2, 8, HD), F32),
        vm((ny - 1, 2, 8, HD), F32),
        vm((ny - 1, 8, HD), F32),
        vm((ny - 1, 8, HD), F32),
        vm((nx, 2, 16, tb), F32),
        vm((1, 3 * block), jnp.int32),
        vm((block, HD), F32),
        vm((block, HD), F32),
        vm((nx, tb, HD), BF16),
        vm((nx, tb, nz * HD), BF16),
        vm((2, tb, nc), BF16),
        vm((2, tb, nc), BF16),
        vm((2, th, nc), BF16),
        vm((2, th, nc), BF16),
        vm((2, th, nc), F32),
        dma((8,)),
        dma, dma((3, 2)),
        dma, dma,
        dma, dma, dma((zh, 2, 3)),
        dma, dma((zh, 2, 2)),
        dma, dma((zh // 2, 2)),
        dma, dma((ny, 2)),
        dma, dma,
        dma, dma,
        dma((2,)), dma((2,)),
        dma, dma((2,)),
        dma, dma((2,)),
        dma, dma((3,)),
        dma, dma((3,)),
        dma, dma((nx, ny - 1)),
        dma, dma((nx,)),
        dma, dma((2, 2)),
        dma, dma((2,)),
    ]
    anywhere = pl.BlockSpec(memory_space=pl.ANY)
    return pl.pallas_call(
        functools.partial(kernel, (ny, nz, tb, kd, nc)),
        out_shape=pltpu.VMEM((tb, nc), BF16),
        in_specs=[anywhere] * 6,
        out_specs=pl.BlockSpec(memory_space=pltpu.VMEM),
        scratch_shapes=scratch,
        compiler_params=pltpu.CompilerParams(
            collective_id=0, has_side_effects=True, vmem_limit_bytes=60 * 2**20
        ),
    )(
        hidden,
        w_query,
        w_keyvalue.T.reshape(2, 16, kd),
        w_output,
        segment_ids.reshape(1, tb),
        jnp.asarray(table),
    )


def solution(mesh):
    ny, nz = mesh.shape["fsdp"] // 2, mesh.shape["sp"] // 4
    split = Mesh(mesh.devices.reshape(ny, 2, nz, 4), ("y", "c", "z", "x"))
    rows, cols = ("z", "x"), ("y", "c")
    placed = (P(rows, cols), P(cols, rows), P(cols, rows), P(rows, cols), P(rows))
    return jax.shard_map(
        functools.partial(on_device, ny, nz),
        mesh=split,
        in_specs=placed,
        out_specs=P(rows, cols),
        check_vma=False,
    )
```

```python
import functools
import math

import jax
import jax.numpy as jnp
import numpy as np
from jax import lax
from jax.experimental import pallas as pl
from jax.experimental.pallas import tpu as pltpu
from jax.sharding import Mesh
from jax.sharding import PartitionSpec as P

HD = 128
HALF = HD // 2
ROPE_BASE = 500000.0
NEG_FILL = -1e30
SEGMENTS = 8
CODES = 32000.0
MESH = pl.DeviceIdType.MESH
F32 = jnp.float32
BF16 = jnp.bfloat16


def dot(a, b):
    return lax.dot_general(a, b, (((1,), (0,)), ((), ())), preferred_element_type=F32)


def dot_nt(a, b):
    return lax.dot_general(a, b, (((1,), (1,)), ((), ())), preferred_element_type=F32)


def kernel(
    dims,
    h_hbm, wq_hbm, wk_hbm, wo_hbm, seg_hbm, freq_hbm, out,
    h, wk, seg, freq, hb, wb, wob, wk2, kvw, pq, rq, pk, rk, sq, yq, acc_q, sk, yk, sk_unit, yk_unit, sq_unit, yq_unit, acc_k,
    seg_win, cos_q, sin_q, qs, mix, send_part, recv_part, relay_out, relay_in, acc_o,
    sem_local, h_s, h_r, sw_s, sw_r, w_s, wk_s, w_r, wo_s, wo_r, d_s, d_r, dk_s, dk_r,
    yq_s, yq_r, yk_s, yk_r, yu_s, yu_r, sg_s, sg_r, kz_s, kz_r, kx_s, kx_r, kc_s, kc_r,
    my_s, my_r, mc_s, mc_r, xr_s, xr_r, xf_s, xf_r,
):
    ny, nz, tb, kd, nc = dims
    nx = 4
    zh = nz // 2
    block = nx * tb
    th = tb // 2
    x = lax.axis_index("x")
    y = lax.axis_index("y")
    z = lax.axis_index("z")
    c = lax.axis_index("c")
    named = jax.named_scope

    def x_at(d):
        return {"x": lax.rem(x + d + nx, nx)}

    def z_at(d):
        return {"z": lax.rem(z + d + nz, nz)}

    def y_at(d):
        return {"y": lax.rem(y + d + ny, ny)}

    partner = {"c": 1 - c}

    def rc(src, dst, ssem, rsem, dev):
        return pltpu.make_async_remote_copy(
            src_ref=src, dst_ref=dst, send_sem=ssem, recv_sem=rsem, device_id=dev, device_id_type=MESH
        )

    def go(cp):
        cp.start()
        return cp

    def whole(ref, ssem, rsem):
        return rc(ref, ref, ssem, rsem, {"c": 1 - c})

    hi = lax.div(x, 2)
    lanes = (pl.ds(0, HD), pl.ds(HD, HD))
    own_lanes = pl.ds(pl.multiple_of(2 * block + x * tb, tb), tb)
    own_rows = pl.ds(pl.multiple_of(z * HD, HD), HD)
    local = {
        "wk": pltpu.make_async_copy(wk_hbm, wk, sem_local.at[0]),
        "wk_own": pltpu.make_async_copy(wk_hbm.at[hi], wk2.at[0, hi], sem_local.at[1]),
        "wq": pltpu.make_async_copy(wq_hbm, wb.at[0, :, lanes[0]], sem_local.at[2]),
        "h": pltpu.make_async_copy(h_hbm, h, sem_local.at[3]),
        "seg": pltpu.make_async_copy(seg_hbm, seg, sem_local.at[4]),
        "seg_own": pltpu.make_async_copy(seg_hbm, seg_win.at[:, own_lanes], sem_local.at[5]),
        "freq": pltpu.make_async_copy(freq_hbm, freq, sem_local.at[6]),
        "wo": pltpu.make_async_copy(wo_hbm, wob.at[own_rows, :], sem_local.at[7]),
    }
    for cp in local.values():
        cp.start()

    barrier = pltpu.get_barrier_semaphore()
    greet = [x_at(d) for d in range(1, nx)] + [z_at(1), z_at(-1), z_at(2), z_at(-2), partner]
    greet += [y_at(d) for d in range(1, ny)]
    for dev in greet:
        pl.semaphore_signal(barrier, inc=1, device_id=dev, device_id_type=MESH)
    for name in ("wk", "wq", "h"):
        local[name].wait()
    with named("barrier"):
        pl.semaphore_wait(barrier, len(greet))

    swap = go(rc(wk.at[1 - hi], wk2.at[0, hi], sw_s, sw_r, x_at(2)))

    k_rows = (pl.ds(0, kd // 2), pl.ds(kd // 2, kd // 2))

    def w_copy(r, way, piece):
        rows = k_rows[piece]
        dst = wb.at[0, rows, lanes[1]] if r == zh else wb.at[r, rows, lanes[1 - way]]
        src = wb.at[0, rows, lanes[0]] if r == 1 else wb.at[r - 1, rows, lanes[1 - way]]
        return rc(src, dst, w_s, w_r.at[r - 1, way, piece], z_at(1 - 2 * way))

    def k_copy(r, way):
        part = pl.ds(0, 2)
        if r == zh:
            part = pl.ds(way, 1)
            dst = wk2.at[zh, part]
        else:
            dst = wk2.at[nz - r if way == 0 else r, part]
        src_at = 0 if r == 1 else (nz - r + 1 if way == 0 else r - 1)
        src = wk2.at[src_at, part]
        return rc(src, dst, wk_s, w_r.at[r - 1, way, 2], z_at(1 - 2 * way))

    def pieces(r, way):
        return (way,) if r == zh else (0, 1)

    w_cp = {}

    def k_step(r):
        for way in range(2):
            w_cp[r, way, 2].wait_recv()
            if r < zh:
                w_cp[r + 1, way, 2] = go(k_copy(r + 1, way))

    def w_step(r, piece):
        for way in range(2):
            if piece in pieces(r, way):
                w_cp[r, way, piece].wait_recv()
                if r < zh and piece in pieces(r + 1, way):
                    w_cp[r + 1, way, piece] = go(w_copy(r + 1, way, piece))

    h_rows = (pl.ds(0, th), pl.ds(th, th))
    for way in range(2):
        w_cp[1, way, 0] = go(w_copy(1, way, 0))
    for k in range(2):
        go(rc(h.at[h_rows[k]], hb.at[2, h_rows[k]], h_s, h_r.at[0, k], x_at(1)))
        go(rc(h.at[h_rows[1 - k]], hb.at[0, h_rows[1 - k]], h_s, h_r.at[1, k], x_at(-1)))

    local["seg"].wait()
    local["seg_own"].wait()
    local["freq"].wait()
    local["wk_own"].wait()

    def seg_x(d):
        return rc(seg, seg_win.at[:, own_lanes], sg_s, sg_r.at[0], x_at(d))

    for d in range(1, nx):
        go(seg_x(d))

    def blk(b):
        return pl.ds((2 - b) * block, block)

    def seg_z(b):
        return rc(seg_win.at[:, blk(0)], seg_win.at[:, blk(b)], sg_s, sg_r.at[1], z_at(b))

    row = lax.broadcasted_iota(jnp.int32, (block, HD), 0)
    pos = (z * block + row).astype(F32)
    angle = pos * freq[4 * 16:4 * 16 + 1, :]
    with named("swap"):
        swap.wait_recv()
    for way in range(2):
        w_cp[1, way, 2] = go(k_copy(1, way))
    for way in range(2):
        w_cp[1, way, 1] = go(w_copy(1, way, 1))
    with named("cos"):
        cos_q[...] = jnp.cos(angle)
    lane = lax.broadcasted_iota(jnp.int32, (block, HD), 1)
    with named("sin"):
        sin_q[...] = jnp.sin(angle) * jnp.where(lane < HALF, -1.0, 1.0)

    def h_recv(way, k):
        rows = h_rows[k] if way == 0 else h_rows[1 - k]
        return rc(h.at[rows], hb.at[2 if way == 0 else 0, rows], h_s, h_r.at[way, k], x_at(1))

    def fwd_hidden(k):
        h_recv(0, k).wait_recv()
        h_recv(1, k).wait_recv()
        if k == 0:
            go(rc(hb.at[2, h_rows[0]], hb.at[1, h_rows[0]], h_s, h_r.at[2, 0], x_at(1)))
            go(rc(hb.at[0, h_rows[1]], hb.at[1, h_rows[1]], h_s, h_r.at[2, 1], x_at(-1)))

    parity = lax.rem(z + c, 2)

    def sub(j):
        return h[...] if j == 0 else hb[j - 1]

    def rows_of(j):
        return pl.ds(pl.multiple_of(lax.rem(x + j, nx) * tb, tb), tb)

    order = (0, 1, 3, 2)
    parts = (pl.ds(0, 3), pl.ds(3, 1))

    def exchange(u, half):
        at = (slice(None), slice(None), lanes[half])
        return rc(pq.at[(u, *at)], rq.at[(u // 2, *at)], d_s, d_r.at[u // 2, half], partner)

    def project(u, js, halves=(0, 1)):
        at = pl.ds(halves[0] * HD, len(halves) * HD)
        for j in js:
            pq[u, order.index(j), :, at] = dot(sub(j), wb[u, :, at])

    def hand_over(u, halves=(0, 1)):
        @pl.when(parity != u % 2)
        def _():
            for half in halves:
                exchange(u, half).start()

    def y_copy(slot, dest):
        return rc(sq.at[slot], yq.at[slot], yq_s, yq_r, {"y": dest})

    def q_unit_y(slot, dest):
        return rc(sq_unit.at[slot], yq_unit.at[slot], yu_s.at[1], yu_r.at[1], {"y": dest})

    def deliver(u, halves=(0, 1)):
        @pl.when(parity == u % 2)
        def _():
            for half in halves:
                exchange(u, half).wait_recv()
                d = (u if half == 0 else (nz - u)) if u else (0 if half == 0 else zh)
                dest = lax.div(lax.rem(z + d, nz), 2)
                slot = lax.rem(y - dest + ny, ny) - 1

                @pl.when(dest == y)
                def _():
                    acc_q[...] = pq[u, :, :, lanes[half]] + rq[u // 2, :, :, lanes[half]]

                @pl.when(dest != y)
                def _():
                    total = pq[u, :, :, lanes[half]] + rq[u // 2, :, :, lanes[half]]
                    largest = jnp.maximum(jnp.max(jnp.abs(total), keepdims=True), 1e-33)
                    sq_unit[slot] = jnp.broadcast_to(largest.reshape(1, 1) * (1.0 / CODES), (8, HD))
                    q_unit_y(slot, dest).start()
                    sq[slot] = jnp.round(total * (CODES / largest)).astype(jnp.int32).astype(jnp.int16)
                    y_copy(slot, dest).start()

    rows_k = nz * 2 * 16

    def k_project(js):
        wk_all = wk2[...].reshape(rows_k, kd)
        for j in js:
            pk[:, order.index(j)] = dot_nt(wk_all, sub(j)).reshape(nz, 2, 16, tb)

    turns = (1, 3, 2, 0)

    def k_chunk(turn, core):
        return lax.rem(2 * lax.rem(y + turn, ny) + core - z + nz, nz)

    def k_exchange(turn, p):
        return rc(
            pk.at[k_chunk(turn, 1 - c), parts[p]], rk.at[turn, parts[p]], dk_s, dk_r.at[turn, p], partner
        )

    def k_hand_over(p):
        for turn in turns:
            k_exchange(turn, p).start()

    def k_copy_y(slot, p, dest):
        return rc(sk.at[slot, parts[p]], yk.at[slot, parts[p]], yk_s, yk_r, {"y": dest})

    def k_unit_y(slot, p, dest):
        return rc(sk_unit.at[slot, p], yk_unit.at[slot, p], yu_s.at[0], yu_r.at[0], {"y": dest})

    def k_deliver(p):
        for turn in turns:
            k_exchange(turn, p).wait_recv()
            dest = lax.rem(y + turn, ny)
            slot = ny - turn - 1
            total = pk[k_chunk(turn, c), parts[p]] + rk[turn, parts[p]]
            if turn == 0:
                acc_k[parts[p]] = total
            else:
                largest = jnp.maximum(jnp.max(jnp.abs(total), keepdims=True), 1e-33)
                sk_unit[slot, p] = jnp.broadcast_to(largest.reshape(1, 1) * (1.0 / CODES), (8, HD))
                k_unit_y(slot, p, dest).start()
                sk[slot, parts[p]] = jnp.round(total * (CODES / largest)).astype(jnp.int32).astype(jnp.int16)
                k_copy_y(slot, p, dest).start()

    def y_other():
        return lax.rem(y + 1, ny)

    o_cols = nc // 2

    def o_copy(r, way, piece):
        owner = lax.rem(z + (nz - r + 1 if way == 0 else r - 1), nz)
        at = wob.at[pl.ds(pl.multiple_of(owner * HD, HD), HD), pl.ds(piece * o_cols, o_cols)]
        return rc(at, at, wo_s, wo_r.at[r - 1, way, piece], z_at(1 - 2 * way))

    def o_step(r, piece, ways=(0, 1)):
        for way in ways:
            if r == 0:
                go(o_copy(1, way, piece))
            elif r < zh or way == 1:
                o_copy(r, way, piece).wait_recv()
                if r + 1 < zh or (r + 1 == zh and way == 1):
                    go(o_copy(r + 1, way, piece))

    early = (0, 1, 3)
    with named("k1"):
        k_step(1)
    with named("w1a"):
        w_step(1, 0)
    with named("hidden0"):
        fwd_hidden(0)
    with named("k2"):
        k_step(2)
    with named("w1b"):
        w_step(1, 1)
    with named("hidden1"):
        fwd_hidden(1)
    with named("project0a"):
        project(0, early, (0,))
    with named("k3"):
        if zh > 3:
            k_step(3)
    with named("w2a"):
        w_step(2, 0)
    with named("project1a"):
        project(1, early)
    whole(seg_win.at[:, pl.ds(0, 3 * tb)], sg_s, sg_r.at[0]).wait_recv()
    for b in (1, 2):
        go(seg_z(b))
    with named("w2b"):
        w_step(2, 1)
    with named("k4"):
        k_step(zh)
    with named("kproject_a"):
        k_project(early)
        k_hand_over(0)
    with named("hidden2"):
        for k in range(2):
            rc(h.at[h_rows[k]], hb.at[1, h_rows[k]], h_s, h_r.at[2, k], x_at(1)).wait_recv()
    with named("kproject_b"):
        k_project((2,))
        k_hand_over(1)
    with named("project1b"):
        project(1, (2,))
        hand_over(1)
    with named("kdeliver_a"):
        k_deliver(0)
    with named("project0b"):
        project(0, (2,), (0,))
        hand_over(0, (0,))
    with named("w3a"):
        w_step(3, 0)
    with named("kdeliver_b"):
        k_deliver(1)
    with named("w3b"):
        if zh > 3:
            w_step(3, 1)
    local["wo"].wait()
    o_step(0, 0)
    o_step(0, 1, (1,))
    with named("project2"):
        project(2, range(nx))
        hand_over(2)
    with named("project3"):
        if zh > 3:
            project(3, range(nx))
            hand_over(3)
    place = 2 * lax.rem(x, 2) + hi
    k_freq = freq[pl.ds(pl.multiple_of(place * 16, 16), 16), 0:1]
    is_key = c == 0
    tables = []
    for j in order:
        first = z * block + lax.rem(x + j, nx) * tb
        k_angle = (first + lax.broadcasted_iota(jnp.int32, (16, tb), 1)).astype(F32) * k_freq
        tables.append((jnp.where(is_key, jnp.cos(k_angle), 1.0), jnp.where(is_key, jnp.sin(k_angle), 0.0)))

    whole(seg_win.at[:, pl.ds(0, 2 * block)], sg_s, sg_r.at[1]).wait_recv()

    wpos = lax.broadcasted_iota(jnp.int32, (1, 3 * block), 1)
    ids = jnp.where(wpos + (z - 2) * block >= 0, seg_win[...], -1)
    starts = [jnp.sum((ids < s).astype(F32), axis=1, keepdims=True).astype(jnp.int32) for s in range(SEGMENTS)]
    with named("deliver10"):
        deliver(1)
        deliver(0, (0,))
    with named("deliver2"):
        deliver(2)
    with named("deliver3"):
        if zh > 3:
            deliver(3)
    with named("ywait_k"):
        whole(yk_unit, yu_s.at[0], yu_r.at[0]).wait_recv()
        whole(yk, yk_s, yk_r).wait_recv()
    for e, j in enumerate(order):
        total = acc_k[e]
        for s in range(ny - 1):
            unit_of = yk_unit[s, 0 if e < 3 else 1][0:1, 0:1].reshape(1, 1, 1)
            total = total + yk[s, e].astype(jnp.int32).astype(F32) * unit_of
        low, high = total[0], total[1]
        cos_e, sin_e = tables[e]
        there = pl.ds(pl.multiple_of(2 * block + lax.rem(x + j, nx) * tb, tb), tb)
        kvw[c, 0, place, :, there] = (low * cos_e - high * sin_e).astype(BF16)
        kvw[c, 1, place, :, there] = (high * cos_e + low * sin_e).astype(BF16)

    def kz(b):
        return rc(kvw.at[c, :, place, :, blk(0)], kvw.at[c, :, place, :, blk(b)], kz_s, kz_r.at[b - 1], z_at(b))

    def kx(b, d):
        at = kvw.at[c, :, place, :, blk(b)]
        return rc(at, at, kx_s, kx_r.at[b], x_at(d))

    def kx_wait(b):
        whole(kvw.at[c, :, pl.ds(0, nx - 1), :, blk(b)], kx_s, kx_r.at[b]).wait_recv()

    def kc(b):
        at = kvw.at[c, :, :, :, blk(b)]
        return rc(at, at, kc_s, kc_r.at[b], partner)

    for b in (1, 2):
        go(kz(b))
    for d in range(1, nx):
        go(kx(0, d))
    o_step(0, 1, (0,))

    with named("w4"):
        for piece in range(2):
            w_step(zh, piece)
    with named("project0c"):
        project(0, range(nx), (1,))
        hand_over(0, (1,))
    with named("deliver0"):
        deliver(0, (1,))
    with named("kz1"):
        kz(1).wait_recv()
    for d in range(1, nx):
        go(kx(1, d))
    with named("o1a"):
        o_step(1, 0)
    with named("kz2"):
        kz(2).wait_recv()
    for d in range(1, nx):
        go(kx(2, d))
    with named("o1b-"):
        o_step(1, 1, (1,))
    with named("kx0"):
        kx_wait(0)
    go(kc(0))
    with named("o2a-"):
        o_step(2, 0, (1,))
    with named("kx1"):
        kx_wait(1)
    go(kc(1))
    with named("o1b+"):
        o_step(1, 1, (0,))
    with named("kx2"):
        kx_wait(2)
    go(kc(2))
    with named("o2b-"):
        o_step(2, 1, (1,))

    with named("ywait_q"):
        whole(yq_unit, yu_s.at[1], yu_r.at[1]).wait_recv()
        whole(yq, yq_s, yq_r).wait_recv()
    with named("rope"):
        for e, j in enumerate(order):
            q = acc_q[e]
            for s in range(ny - 1):
                q = q + yq[s, e].astype(jnp.int32).astype(F32) * yq_unit[s][0:1, 0:1]
            qs[e] = (q * cos_q[rows_of(j)] + pltpu.roll(q, HALF, 1) * sin_q[rows_of(j)]).astype(BF16)
    reach = 2 * block + tb
    unit = HD**-0.5 * math.log2(math.e)
    f = 2 * y + c
    own_f = pl.ds(pl.multiple_of(f * HD, HD), HD)
    with named("kcwait"):
        for b in (0, 1, 2):
            kc(b).wait_recv()

    def attend(j, rows=None):
        first, count = (0, tb) if rows is None else (rows * th, th)
        t = lax.rem(x + j, nx)
        at = pl.multiple_of(t * tb, tb)
        q = qs[order.index(j), pl.ds(first, count)]
        keys = kvw[0, :, :, :, pl.ds(at, reach)].reshape(HD, reach)
        values = kvw[1, :, :, :, pl.ds(at, reach)].reshape(HD, reach)
        scores = dot(q, keys) * unit
        here = lax.broadcasted_iota(jnp.int32, (count, 1), 0) + (2 * block + first)
        begin = jnp.zeros((count, 1), jnp.int32)
        for s in starts:
            begin = jnp.maximum(begin, jnp.where(s - at <= here, s - at, 0))
        k_at = lax.broadcasted_iota(jnp.int32, (count, reach), 1)
        ahead, own = slice(0, 2 * block), slice(2 * block, reach)
        scores = jnp.concatenate(
            [
                jnp.where(k_at[:, ahead] >= begin, scores[:, ahead], NEG_FILL),
                jnp.where((k_at[:, own] >= begin) & (k_at[:, own] <= here), scores[:, own], NEG_FILL),
            ],
            axis=1,
        )
        top = jnp.max(scores, axis=1, keepdims=True)
        weights = jnp.exp2(scores - top)
        total = jnp.sum(weights, axis=1, keepdims=True)
        mixed = dot_nt(weights.astype(BF16), values)
        mix[j, pl.ds(first, count), own_f] = (mixed / total).astype(BF16)
        for d in range(1, ny):
            go(my(j, d, rows))
        if rows != 0:
            go(mc(j, 0))

    def my(j, d, rows=None):
        at = mix.at[j, :, own_f] if rows is None else mix.at[j, pl.ds(rows * th, th), own_f]
        return rc(at, at, my_s, my_r.at[j if rows != 0 else nx, d - 1], y_at(d))

    def mc(j, d):
        fd = 2 * lax.rem(y - d + ny, ny) + c
        at = mix.at[j, :, pl.ds(pl.multiple_of(fd * HD, HD), HD)]
        return rc(at, at, mc_s, mc_r.at[j], partner)

    def pass_mix(j):
        for d in range(1, ny):
            if j == 2:
                my(j, d, 0).wait_recv()
            my(j, d, 1 if j == 2 else None).wait_recv()
            go(mc(j, d))

    def have_mix(j):
        whole(mix.at[j, :, pl.ds(0, ny * HD)], mc_s, mc_r.at[j]).wait_recv()

    def half_of(k):
        return pl.ds(k * th, th)

    def cols(i):
        return pl.ds(i * o_cols, o_cols)

    def relay(k, i):
        return rc(relay_out.at[k, :, cols(i)], relay_in.at[k, :, cols(i)], xr_s, xr_r.at[k, i], x_at(1 - 2 * k))

    def final(k, part, i):
        at = (k, half_of(1 - k) if part == 0 else half_of(k), cols(i))
        return rc(send_part.at[at], recv_part.at[at], xf_s, xf_r.at[i], x_at(1 - 2 * k))

    def out_dot(j, k, i):
        return dot(mix[j, half_of(k)], wob[:, cols(i)])

    with named("att2"):
        attend(2, 0)
        attend(2, 1)
    with named("o2a+"):
        o_step(2, 0, (0,))
    with named("o3a-"):
        o_step(3, 0, (1,))
    with named("att1"):
        attend(1)
    with named("o2b+"):
        o_step(2, 1, (0,))
    with named("o3b-"):
        o_step(3, 1, (1,))
    with named("att3"):
        attend(3)
    with named("gm2"):
        pass_mix(2)
    with named("o4a"):
        o_step(3, 0, (0,))
        o_step(zh, 0)
    with named("mix2"):
        have_mix(2)
    with named("mm2"):
        for k in range(2):
            relay_out[k, :, cols(0)] = out_dot(2, k, 0).astype(BF16)
            go(relay(k, 0))
    with named("o4b"):
        o_step(3, 1, (0,))
        o_step(zh, 1)
    with named("mm2"):
        for k in range(2):
            relay_out[k, :, cols(1)] = out_dot(2, k, 1).astype(BF16)
            go(relay(k, 1))
    with named("gm1"):
        pass_mix(1)
    with named("att0"):
        attend(0)
    with named("mm1"):
        have_mix(1)
        for i in range(2):
            send_part[0, half_of(1), cols(i)] = out_dot(1, 1, i).astype(BF16)
            go(final(0, 0, i))
    with named("gm3"):
        pass_mix(3)
        have_mix(3)
    with named("mm3"):
        for i in range(2):
            send_part[1, half_of(0), cols(i)] = out_dot(3, 0, i).astype(BF16)
            go(final(1, 0, i))
    with named("mm31"):
        for i in range(2):
            for k, j in ((0, 1), (1, 3)):
                acc_o[k, :, cols(i)] = out_dot(j, k, i)
        pass_mix(0)
    for i in range(2):
        for k in range(2):
            with named("relay"):
                relay(k, i).wait_recv()
            send_part[k, half_of(k), cols(i)] = (acc_o[k, :, cols(i)] + relay_in[k, :, cols(i)].astype(F32)).astype(BF16)
            go(final(k, 1, i))
    with named("mm0"):
        have_mix(0)
        for i in range(2):
            for k in range(2):
                acc_o[k, :, cols(i)] = out_dot(0, k, i)

    with named("drain"):
        for ref, ssem, rsem in (
            (hb, h_s, h_r.at[0, 0]),
            (wk.at[0], sw_s, sw_r),
            (wb.at[:, pl.ds(0, kd - kd // 8)], w_s, w_r.at[0, 0, 0]),
            (wk2.at[pl.ds(0, nz - 1)], wk_s, w_r.at[0, 0, 0]),
            (wob.at[pl.ds(0, (nz - 1) * HD)], wo_s, wo_r.at[0, 0, 0]),
            (rq, d_s, d_r.at[0, 0]),
            (rk, dk_s, dk_r.at[0, 0]),
            (yq, yq_s, yq_r),
            (seg_win.at[:, pl.ds(0, 3 * tb + 2 * block)], sg_s, sg_r.at[0]),
            (kvw.at[0, :, pl.ds(0, 2), :, blk(0)], kz_s, kz_r.at[0]),
            (kvw.at[0, :, pl.ds(0, 3)], kx_s, kx_r.at[0]),
            (kvw.at[0], kc_s, kc_r.at[0]),
            (mix.at[pl.ds(0, 3), half_of(0)], my_s, my_r.at[0, 0]),
            (mix.at[pl.ds(0, 2)], mc_s, mc_r.at[0]),
            (relay_out, xr_s, xr_r.at[0, 0]),
            (send_part, xf_s, xf_r.at[0]),
        ):
            whole(ref, ssem, rsem).wait_send()

        whole(yk, yk_s, yk_r).wait_send()
        whole(yk_unit, yu_s.at[0], yu_r.at[0]).wait_send()
        whole(yq_unit, yu_s.at[1], yu_r.at[1]).wait_send()
    for i in range(2):
        with named("final"):
            whole(recv_part.at[:, :, cols(i)], xf_s, xf_r.at[i]).wait_recv()
        for k in range(2):
            rows = half_of(k)
            out[rows, cols(i)] = (
                acc_o[k, :, cols(i)] + recv_part[0, rows, cols(i)].astype(F32) + recv_part[1, rows, cols(i)].astype(F32)
            ).astype(BF16)


def on_device(ny, nz, hidden, w_query, w_keyvalue, w_output, segment_ids):
    tb, kd = hidden.shape
    nc = w_output.shape[1]
    nx, zh, block, th = 4, nz // 2, 4 * hidden.shape[0], hidden.shape[0] // 2
    freq = np.exp(np.arange(HALF, dtype=np.float32) * np.float32(-2.0 * math.log(ROPE_BASE) / HD))
    table = np.zeros((72, HD), np.float32)
    table[:HALF, 0] = freq
    table[HALF] = np.concatenate([freq, freq])
    dma = pltpu.SemaphoreType.DMA
    vm = pltpu.VMEM
    scratch = [
        vm((tb, kd), BF16),
        vm((2, 16, kd), BF16),
        vm((1, tb), jnp.int32),
        vm((72, HD), F32),
        vm((3, tb, kd), BF16),
        vm((zh, kd, 2 * HD), BF16),
        vm((nz * HD, nc), BF16),
        vm((nz, 2, 16, kd), BF16),
        vm((2, 2, 4, 16, 3 * block), BF16),
        vm((zh, nx, tb, 2 * HD), F32),
        vm((zh // 2, nx, tb, 2 * HD), F32),
        vm((nz, nx, 2, 16, tb), F32),
        vm((nz // 2, nx, 2, 16, tb), F32),
        vm((ny - 1, nx, tb, HD), jnp.int16),
        vm((ny - 1, nx, tb, HD), jnp.int16),
        vm((nx, tb, HD), F32),
        vm((ny - 1, nx, 2, 16, tb), jnp.int16),
        vm((ny - 1, nx, 2, 16, tb), jnp.int16),
        vm((ny - 1, 2, 8, HD), F32),
        vm((ny - 1, 2, 8, HD), F32),
        vm((ny - 1, 8, HD), F32),
        vm((ny - 1, 8, HD), F32),
        vm((nx, 2, 16, tb), F32),
        vm((1, 3 * block), jnp.int32),
        vm((block, HD), F32),
        vm((block, HD), F32),
        vm((nx, tb, HD), BF16),
        vm((nx, tb, nz * HD), BF16),
        vm((2, tb, nc), BF16),
        vm((2, tb, nc), BF16),
        vm((2, th, nc), BF16),
        vm((2, th, nc), BF16),
        vm((2, th, nc), F32),
        dma((8,)),
        dma, dma((3, 2)),
        dma, dma,
        dma, dma, dma((zh, 2, 3)),
        dma, dma((zh, 2, 2)),
        dma, dma((zh // 2, 2)),
        dma, dma((ny, 2)),
        dma, dma,
        dma, dma,
        dma((2,)), dma((2,)),
        dma, dma((2,)),
        dma, dma((2,)),
        dma, dma((3,)),
        dma, dma((3,)),
        dma, dma((nx + 1, ny - 1)),
        dma, dma((nx,)),
        dma, dma((2, 2)),
        dma, dma((2,)),
    ]
    anywhere = pl.BlockSpec(memory_space=pl.ANY)
    return pl.pallas_call(
        functools.partial(kernel, (ny, nz, tb, kd, nc)),
        out_shape=pltpu.VMEM((tb, nc), BF16),
        in_specs=[anywhere] * 6,
        out_specs=pl.BlockSpec(memory_space=pltpu.VMEM),
        scratch_shapes=scratch,
        compiler_params=pltpu.CompilerParams(
            collective_id=0, has_side_effects=True, vmem_limit_bytes=60 * 2**20
        ),
    )(
        hidden,
        w_query,
        w_keyvalue.T.reshape(2, 16, kd),
        w_output,
        segment_ids.reshape(1, tb),
        jnp.asarray(table),
    )


def solution(mesh):
    ny, nz = mesh.shape["fsdp"] // 2, mesh.shape["sp"] // 4
    split = Mesh(mesh.devices.reshape(ny, 2, nz, 4), ("y", "c", "z", "x"))
    rows, cols = ("z", "x"), ("y", "c")
    placed = (P(rows, cols), P(cols, rows), P(cols, rows), P(rows, cols), P(rows))
    return jax.shard_map(
        functools.partial(on_device, ny, nz),
        mesh=split,
        in_specs=placed,
        out_specs=P(rows, cols),
        check_vma=False,
    )
```
